32 devices in a mesh: rows: 8 (over z, x), bal: 4 (over y, core).
Axes of the slice: x: 2, y: 2, z: 4, core: 2. Of those that a mesh axis runs over, the one named last changes fastest.
Arguments:
- embeddings: bfloat16 [16384, 1024], P(('rows', 'bal')), may hold values from -60 to 60
- cluster_blocks: int32 [16], replicated, may hold values from 1 to 4, as said below
Outputs:
- row_max: float32 [16384], P(('rows', 'bal'))
The draws below stay inside these ranges and needn't reach their ends.
Inputs may be any that keep to these rules, and one draw needn't show every extreme that they name: `cluster_blocks`: the sizes sum to 32; at least one cluster has exactly 4 blocks.
All inputs are finite; a program needn't handle non-finite values.
Results may differ from the reference program's by a relative error of at most 0.00051.
Values may be sent and summed in bfloat16 or wider, within the bound.
A program may use at most 64 MiB of HBM per device.

```python
import jax
import jax.numpy as jnp
from jax import lax

D = 1024
BLOCK = 512
MAXB = 4
NBLK = 32
NCL = 16


def fill_segment(sizes, key, first, last, extra):
    slots = jnp.arange(NCL, dtype=jnp.int32)
    picks = jax.random.randint(jax.random.fold_in(key, 22), (extra,), 0, NCL)
    shuffled = jax.random.permutation(jax.random.fold_in(key, 23), NCL).astype(jnp.int32)
    outside = ((slots < first) | (slots >= last)).astype(jnp.int32)

    def place(counts, pick):
        biased = shuffled[pick * pick // NCL]
        distance = (slots - biased) % NCL
        blocked = jnp.maximum((counts >= MAXB).astype(jnp.int32), outside)
        target = jnp.argmin(distance + NCL * blocked)
        return (counts.at[target].add(1), 0)
    sizes, _ = lax.scan(place, sizes, picks)
    return sizes


def cluster_sizes(key):
    special = NCL // 2
    sizes = jnp.ones((NCL,), jnp.int32).at[special].set(MAXB)
    front_extra = NBLK // 2 - 2 - special
    back_extra = NBLK - NBLK // 2 - 2 - (NCL - special - 1)
    sizes = fill_segment(sizes, jax.random.fold_in(key, 41), 0, special, front_extra)
    sizes = fill_segment(sizes, jax.random.fold_in(key, 42), special + 1, NCL, back_extra)
    return sizes


def draw_cluster_blocks(key, part):
    return cluster_sizes(jax.random.fold_in(key, 7))


def draw_embeddings(key, part):
    sizes = cluster_sizes(jax.random.fold_in(key, 7))
    bounds = jnp.cumsum(sizes)
    starts = bounds - sizes
    blocks_all = jnp.arange(NBLK, dtype=jnp.int32)
    owner = jnp.sum((bounds[None, :] <= blocks_all[:, None]).astype(jnp.int32), axis=1)
    first_block = starts[owner]
    span_blocks = sizes[owner]
    total_rows = NBLK * BLOCK
    row_block = jnp.arange(total_rows, dtype=jnp.int32) // BLOCK
    jumps = jax.random.randint(jax.random.fold_in(key, 31), (total_rows,), 0, MAXB * BLOCK)
    partner_block = first_block[row_block] + jumps // BLOCK % span_blocks[row_block]
    partner_row = partner_block * BLOCK + jumps % BLOCK
    weight_dup = jax.random.uniform(jax.random.fold_in(key, 33), (total_rows, 1), jnp.float32, 0.3, 2.0)
    base = jnp.clip(jax.random.normal(jax.random.fold_in(key, 32), (total_rows, D), jnp.float32), -6.0, 6.0)
    mixed = base + weight_dup * base[partner_row]
    return mixed.astype(jnp.bfloat16)


def setup_inputs(seed: int = 0) -> dict:
    key_list = jax.random.split(jax.random.key(seed), 3)
    embeddings = draw_embeddings(jax.random.fold_in(key_list[2], 71), 0)
    cluster_blocks = draw_cluster_blocks(jax.random.fold_in(key_list[2], 71), 0)
    return {"embeddings": embeddings, "cluster_blocks": cluster_blocks}


EPSILON = 1e-06

def unit_rows(block_rows):
    values = block_rows.astype(jnp.float32)
    scaled = values * lax.rsqrt(lax.optimization_barrier(jnp.sum(values * values, axis=1, keepdims=True)) + EPSILON)
    return scaled.astype(jnp.bfloat16)

def reference(embeddings, cluster_blocks):
    blocks_all = embeddings.shape[0] // BLOCK
    normed = unit_rows(embeddings).astype(jnp.float32).reshape(blocks_all, BLOCK, D)
    bounds = jnp.cumsum(cluster_blocks).astype(jnp.int32)
    positions = jnp.arange(blocks_all, dtype=jnp.int32)
    diagonal_mask = jnp.arange(BLOCK)[:, None] == jnp.arange(BLOCK)[None, :]
    highest = jnp.full((blocks_all, BLOCK), -2.0, jnp.float32)
    for offset in range(MAXB):
        if offset == 0:
            partner = normed
        else:
            partner = jnp.concatenate([jnp.zeros((offset, BLOCK, D), jnp.float32), normed[:-offset]], axis=0)
        lower = positions - offset
        crossing = lax.optimization_barrier(jnp.sum(((bounds[None, :] > lower[:, None]) & (bounds[None, :] <= positions[:, None])).astype(jnp.int32), axis=1))
        allowed = (lower >= 0) & (crossing == 0)

        def tile(items):
            mine, theirs, permitted = items
            products = jnp.dot(mine, theirs.T, precision=lax.Precision.HIGHEST)
            products = jnp.where(permitted, products, -2.0)
            if offset == 0:
                products = jnp.where(diagonal_mask, -2.0, products)
            return (lax.optimization_barrier(jnp.max(products, axis=1)), lax.optimization_barrier(jnp.max(products, axis=0)))
        row_part, col_part = lax.map(tile, (normed, partner, allowed))
        highest = jnp.maximum(highest, row_part)
        if offset > 0:
            returned = jnp.concatenate([col_part[offset:], jnp.full((offset, BLOCK), -2.0, jnp.float32)], axis=0)
            highest = jnp.maximum(highest, returned)
    return highest.reshape(-1)
```

```python
import functools

import jax
import jax.numpy as jnp
from jax import lax
from jax.experimental import pallas as pl
from jax.experimental.pallas import tpu as pltpu
from jax.sharding import PartitionSpec as P

EPSILON = 1e-06
LOW = -2.0
MESH_ID = pl.DeviceIdType.MESH
PIECES = 8


def nearest_kernel(sizes, counts_ref, x_ref, out_ref, raw, pair, two_back, three_back,
                   row_two, row_three, best, part_out, ret_out, ret3_out, part_in, ret_in, ret3_in,
                   load_sem, pair_send, pair_recv, two_send, two_recv, three_send, three_recv,
                   small_send, small_recv):
    n_rows, n_bal = sizes
    total = n_rows * n_bal
    block, width = x_ref.shape
    piece = block // PIECES
    me = lax.axis_index("rows") * n_bal + lax.axis_index("bal")
    odd = lax.rem(me, 2)
    quarter = lax.rem(me, 4)
    partner = me + 1 - 2 * odd
    is_even = odd == 0
    is_odd = odd == 1

    has_later = me + 2 < total
    has_earlier = me >= 2
    has_later3 = is_odd & (me + 3 < total)
    has_earlier3 = is_even & (me >= 3)
    sends_direct = has_later & ((quarter != 3) | (me + 3 >= total))
    relays = has_earlier3 & (quarter == 2)
    relayed_to = has_earlier & (quarter == 1) & (me + 1 < total)

    def coords(index):
        return (index // n_bal, lax.rem(index, n_bal))

    barrier = pltpu.get_barrier_semaphore()
    greeted = jnp.int32(0)
    for there, index in (
        (me >= 0, partner),
        (has_later, me + 2),
        (has_earlier, me - 2),
        (has_later3, me + 3),
        (has_earlier3, me - 3),
        (relays, me - 1),
        (relayed_to, me + 1),
    ):
        @pl.when(there)
        def _():
            pl.semaphore_signal(barrier, inc=1, device_id=coords(index), device_id_type=MESH_ID)
        greeted = greeted + there.astype(jnp.int32)

    load = pltpu.make_async_copy(x_ref, raw, load_sem)
    load.start()

    def count(i, carry):
        end, crossings = carry
        end = end + counts_ref[i]
        found = []
        for (lower, upper), old in zip(spans, crossings):
            found.append(old + ((end > lower) & (end <= upper)).astype(jnp.int32))
        return end, tuple(found)

    spans = ((me - 3, me), (me - 2, me), (me - 1, me), (me, me + 1), (me - 2, partner))
    zero = jnp.int32(0)
    _, crossings = lax.fori_loop(0, counts_ref.shape[0], count, (zero, (zero,) * len(spans)))
    near3 = crossings[0] == 0
    near2 = crossings[1] == 0
    near_partner = jnp.where(is_odd, crossings[2], crossings[3]) == 0
    near2_partner = crossings[4] == 0

    load.wait()

    @pl.loop(0, PIECES)
    def _(q):
        rows = pl.ds(pl.multiple_of(q * piece, piece), piece)
        values = raw[rows, :].astype(jnp.float32)
        scale = lax.rsqrt(jnp.sum(values * values, axis=1, keepdims=True) + EPSILON)
        pair[0, rows, :] = (values * scale).astype(jnp.bfloat16)

    pl.semaphore_wait(barrier, greeted)

    def rows_of(q):
        return pl.ds(pl.multiple_of(q * piece, piece), piece)

    def to_two(q):
        return pltpu.make_async_remote_copy(
            src_ref=pair.at[0, rows_of(q)], dst_ref=two_back.at[rows_of(q)],
            send_sem=two_send.at[q], recv_sem=two_recv.at[q],
            device_id=coords(me + 2), device_id_type=MESH_ID)

    def to_three(q):
        return pltpu.make_async_remote_copy(
            src_ref=pair.at[0, rows_of(q)], dst_ref=three_back.at[rows_of(q)],
            send_sem=three_send.at[q], recv_sem=three_recv.at[q],
            device_id=coords(me + 3), device_id_type=MESH_ID)

    def onward(q):
        return pltpu.make_async_remote_copy(
            src_ref=three_back.at[rows_of(q)], dst_ref=two_back.at[rows_of(q)],
            send_sem=three_send.at[q], recv_sem=two_recv.at[q],
            device_id=coords(me - 1), device_id_type=MESH_ID)

    def to_partner():
        return pltpu.make_async_remote_copy(
            src_ref=pair.at[0], dst_ref=pair.at[1],
            send_sem=pair_send, recv_sem=pair_recv,
            device_id=coords(partner), device_id_type=MESH_ID)

    def small(slot, src, dst, index):
        return pltpu.make_async_remote_copy(
            src_ref=src, dst_ref=dst, send_sem=small_send.at[slot], recv_sem=small_recv.at[slot],
            device_id=coords(index), device_id_type=MESH_ID)

    to_partner().start()

    @pl.loop(0, PIECES)
    def _(q):
        @pl.when(has_later3)
        def _():
            to_three(q).start()

        @pl.when(sends_direct)
        def _():
            to_two(q).start()

    def products(left, right):
        return lax.dot_general(left, right, (((1,), (1,)), ((), ())),
                               preferred_element_type=jnp.float32)

    step = 128
    best[...] = jnp.full(best.shape, LOW, jnp.float32)

    @pl.loop(0, block // step)
    def _(s):
        rows = pl.ds(pl.multiple_of(s * step, step), step)
        own = products(pair[0, rows, :], pair[0])
        across = lax.broadcasted_iota(jnp.int32, own.shape, 1)
        down = lax.broadcasted_iota(jnp.int32, own.shape, 0) + s * step
        own = jnp.where(across == down, LOW, own)
        best[0:1, :] = jnp.maximum(best[0:1, :], jnp.max(own, axis=0, keepdims=True))

    to_partner().wait()

    @pl.loop(0, block // step)
    def _(s):
        rows = pl.ds(pl.multiple_of(s * step, step), step)
        other = products(pair[1, rows, :], pair[0])
        top = jnp.max(other, axis=0, keepdims=True)
        best[0:1, :] = jnp.maximum(best[0:1, :], jnp.where(near_partner, top, LOW))

    def lanes_max(tile):
        highest = tile[:, :128]
        for start in range(128, tile.shape[1], 128):
            highest = jnp.maximum(highest, tile[:, start:start + 128])
        return highest

    @pl.loop(0, PIECES)
    def _(q):
        rows = rows_of(q)

        @pl.when(has_earlier3)
        def _():
            to_three(q).wait_recv()

            @pl.when(relays)
            def _():
                onward(q).start()

            tile = products(three_back[rows, :], pair[0])
            row_three[rows, :] = lanes_max(tile)
            top = jnp.max(tile, axis=0, keepdims=True)
            best[0:1, :] = jnp.maximum(best[0:1, :], jnp.where(near3, top, LOW))

        @pl.when(has_earlier)
        def _():
            to_two(q).wait_recv()
            tile = products(two_back[rows, :], pair[0])
            other = products(two_back[rows, :], pair[1])
            row_two[rows, :] = jnp.maximum(
                jnp.where(near2, lanes_max(tile), LOW),
                jnp.where(near2_partner, lanes_max(other), LOW))
            top = jnp.max(tile, axis=0, keepdims=True)
            best[0:1, :] = jnp.maximum(best[0:1, :], jnp.where(near2, top, LOW))
            top = jnp.max(other, axis=0, keepdims=True)
            best[1:2, :] = jnp.maximum(best[1:2, :], jnp.where(near2_partner, top, LOW))

    @pl.when(has_earlier)
    def _():
        ret_out[...] = jnp.max(row_two[...].T, axis=0, keepdims=True)
        part_out[...] = best[1:2, :]
        small(0, ret_out, ret_in, me - 2).start()
        small(1, part_out, part_in, partner).start()

    @pl.when(has_earlier3)
    def _():
        top = jnp.max(row_three[...].T, axis=0, keepdims=True)
        ret3_out[...] = jnp.where(near3, top, LOW)
        small(2, ret3_out, ret3_in, me - 3).start()

    @pl.when(has_earlier)
    def _():
        small(1, part_out, part_in, partner).wait()
        best[0:1, :] = jnp.maximum(best[0:1, :], part_in[...])

    @pl.when(has_later3)
    def _():
        small(2, ret3_out, ret3_in, me + 3).wait_recv()
        best[0:1, :] = jnp.maximum(best[0:1, :], ret3_in[...])

    @pl.when(has_later)
    def _():
        small(0, ret_out, ret_in, me + 2).wait_recv()
        best[0:1, :] = jnp.maximum(best[0:1, :], ret_in[...])

    out_ref[...] = best[0:1, :]

    @pl.loop(0, PIECES)
    def _(q):
        @pl.when(has_later3)
        def _():
            to_three(q).wait_send()

        @pl.when(sends_direct)
        def _():
            to_two(q).wait_send()

        @pl.when(relays)
        def _():
            onward(q).wait_send()

    @pl.when(has_earlier)
    def _():
        small(0, ret_out, ret_in, me - 2).wait_send()

    @pl.when(has_earlier3)
    def _():
        small(2, ret3_out, ret3_in, me - 3).wait_send()


def shards(sizes, embeddings, cluster_blocks):
    block, width = embeddings.shape
    line = pltpu.VMEM((1, block), jnp.float32)
    wide = pltpu.VMEM((block, width), jnp.bfloat16)
    flags = pltpu.SemaphoreType.DMA((PIECES,))
    lone = pltpu.SemaphoreType.DMA
    out = pl.pallas_call(
        functools.partial(nearest_kernel, sizes),
        out_shape=jax.ShapeDtypeStruct((1, block), jnp.float32),
        in_specs=[pl.BlockSpec(memory_space=pltpu.SMEM), pl.BlockSpec(memory_space=pl.ANY)],
        out_specs=pl.BlockSpec(memory_space=pltpu.VMEM),
        scratch_shapes=[
            wide, pltpu.VMEM((2, block, width), jnp.bfloat16), wide, wide,
            pltpu.VMEM((block, 128), jnp.float32), pltpu.VMEM((block, 128), jnp.float32),
            pltpu.VMEM((8, block), jnp.float32),
            line, line, line, line, line, line,
            lone, lone, lone, flags, flags, flags, flags,
            pltpu.SemaphoreType.DMA((3,)), pltpu.SemaphoreType.DMA((3,)),
        ],
        compiler_params=pltpu.CompilerParams(collective_id=0, has_side_effects=True),
        name="nearest",
    )(cluster_blocks, embeddings)
    return out.reshape(-1)


def solution(mesh):
    sizes = (mesh.shape["rows"], mesh.shape["bal"])
    return jax.shard_map(
        functools.partial(shards, sizes), mesh=mesh,
        in_specs=(P(("rows", "bal"), None), P()), out_specs=P(("rows", "bal")), check_vma=False)
```

```python
import functools

import jax
import jax.numpy as jnp
from jax import lax
from jax.experimental import pallas as pl
from jax.experimental.pallas import tpu as pltpu
from jax.sharding import PartitionSpec as P

EPSILON = 1e-06
LOW = -2.0
MESH_ID = pl.DeviceIdType.MESH
PIECES = 8


def nearest_kernel(sizes, counts_hbm, x_ref, out_ref, raw, pair, two_back, three_back,
                   row_two, row_three, best, part_out, ret_out, ret3_out, part_in, ret_in, ret3_in,
                   load_sem, pair_send, pair_recv, two_send, two_recv, three_send, three_recv,
                   small_send, small_recv, counts_ref, counts_sem):
    n_rows, n_bal = sizes
    total = n_rows * n_bal
    block, width = x_ref.shape
    piece = block // PIECES
    me = lax.axis_index("rows") * n_bal + lax.axis_index("bal")
    odd = lax.rem(me, 2)
    quarter = lax.rem(me, 4)
    partner = me + 1 - 2 * odd
    is_even = odd == 0
    is_odd = odd == 1

    has_later = me + 2 < total
    has_earlier = me >= 2
    has_later3 = is_odd & (me + 3 < total)
    has_earlier3 = is_even & (me >= 3)
    sends_direct = has_later & ((quarter != 3) | (me + 3 >= total))
    relays = has_earlier3 & (quarter == 2)
    relayed_to = has_earlier & (quarter == 1) & (me + 1 < total)

    def coords(index):
        return (index // n_bal, lax.rem(index, n_bal))

    barrier = pltpu.get_barrier_semaphore()
    greeted = jnp.int32(0)
    for there, index in (
        (me >= 0, partner),
        (has_later, me + 2),
        (has_earlier, me - 2),
        (has_later3, me + 3),
        (has_earlier3, me - 3),
        (relays, me - 1),
        (relayed_to, me + 1),
    ):
        @pl.when(there)
        def _():
            pl.semaphore_signal(barrier, inc=1, device_id=coords(index), device_id_type=MESH_ID)
        greeted = greeted + there.astype(jnp.int32)

    load = pltpu.make_async_copy(x_ref, raw, load_sem)
    load.start()
    counts_load = pltpu.make_async_copy(counts_hbm, counts_ref, counts_sem)
    counts_load.start()

    load.wait()

    @pl.loop(0, PIECES)
    def _(q):
        rows = pl.ds(pl.multiple_of(q * piece, piece), piece)
        values = raw[rows, :].astype(jnp.float32)
        scale = lax.rsqrt(jnp.sum(values * values, axis=1, keepdims=True) + EPSILON)
        pair[0, rows, :] = (values * scale).astype(jnp.bfloat16)

    pl.semaphore_wait(barrier, greeted)

    def rows_of(q):
        return pl.ds(pl.multiple_of(q * piece, piece), piece)

    def to_two(q):
        return pltpu.make_async_remote_copy(
            src_ref=pair.at[0, rows_of(q)], dst_ref=two_back.at[rows_of(q)],
            send_sem=two_send.at[q], recv_sem=two_recv.at[q],
            device_id=coords(me + 2), device_id_type=MESH_ID)

    def to_three(q):
        return pltpu.make_async_remote_copy(
            src_ref=pair.at[0, rows_of(q)], dst_ref=three_back.at[rows_of(q)],
            send_sem=three_send.at[q], recv_sem=three_recv.at[q],
            device_id=coords(me + 3), device_id_type=MESH_ID)

    def onward(q):
        return pltpu.make_async_remote_copy(
            src_ref=three_back.at[rows_of(q)], dst_ref=two_back.at[rows_of(q)],
            send_sem=three_send.at[q], recv_sem=two_recv.at[q],
            device_id=coords(me - 1), device_id_type=MESH_ID)

    def to_partner():
        return pltpu.make_async_remote_copy(
            src_ref=pair.at[0], dst_ref=pair.at[1],
            send_sem=pair_send, recv_sem=pair_recv,
            device_id=coords(partner), device_id_type=MESH_ID)

    def small(slot, src, dst, index):
        return pltpu.make_async_remote_copy(
            src_ref=src, dst_ref=dst, send_sem=small_send.at[slot], recv_sem=small_recv.at[slot],
            device_id=coords(index), device_id_type=MESH_ID)

    to_partner().start()

    @pl.loop(0, PIECES)
    def _(q):
        @pl.when(has_later3)
        def _():
            to_three(q).start()

        @pl.when(sends_direct)
        def _():
            to_two(q).start()

    counts_load.wait()

    def count(i, carry):
        end, crossings = carry
        end = end + counts_ref[i]
        found = []
        for (lower, upper), old in zip(spans, crossings):
            found.append(old + ((end > lower) & (end <= upper)).astype(jnp.int32))
        return end, tuple(found)

    spans = ((me - 3, me), (me - 2, me), (me - 1, me), (me, me + 1), (me - 2, partner))
    zero = jnp.int32(0)
    _, crossings = lax.fori_loop(0, counts_ref.shape[0], count, (zero, (zero,) * len(spans)))
    near3 = crossings[0] == 0
    near2 = crossings[1] == 0
    near_partner = jnp.where(is_odd, crossings[2], crossings[3]) == 0
    near2_partner = crossings[4] == 0

    def products(left, right):
        return lax.dot_general(left, right, (((1,), (1,)), ((), ())),
                               preferred_element_type=jnp.float32)

    step = 128
    best[...] = jnp.full(best.shape, LOW, jnp.float32)

    @pl.loop(0, block // step)
    def _(s):
        rows = pl.ds(pl.multiple_of(s * step, step), step)
        own = products(pair[0, rows, :], pair[0])
        across = lax.broadcasted_iota(jnp.int32, own.shape, 1)
        down = lax.broadcasted_iota(jnp.int32, own.shape, 0) + s * step
        own = jnp.where(across == down, LOW, own)
        best[0:1, :] = jnp.maximum(best[0:1, :], jnp.max(own, axis=0, keepdims=True))

    to_partner().wait()

    @pl.loop(0, block // step)
    def _(s):
        rows = pl.ds(pl.multiple_of(s * step, step), step)
        other = products(pair[1, rows, :], pair[0])
        top = jnp.max(other, axis=0, keepdims=True)
        best[0:1, :] = jnp.maximum(best[0:1, :], jnp.where(near_partner, top, LOW))

    def lanes_max(tile):
        highest = tile[:, :128]
        for start in range(128, tile.shape[1], 128):
            highest = jnp.maximum(highest, tile[:, start:start + 128])
        return highest

    @pl.loop(0, PIECES)
    def _(q):
        rows = rows_of(q)

        @pl.when(has_earlier3)
        def _():
            to_three(q).wait_recv()

            @pl.when(relays)
            def _():
                onward(q).start()

            tile = products(three_back[rows, :], pair[0])
            row_three[rows, :] = lanes_max(tile)
            top = jnp.max(tile, axis=0, keepdims=True)
            best[0:1, :] = jnp.maximum(best[0:1, :], jnp.where(near3, top, LOW))

        @pl.when(has_earlier)
        def _():
            to_two(q).wait_recv()
            tile = products(two_back[rows, :], pair[0])
            other = products(two_back[rows, :], pair[1])
            row_two[rows, :] = jnp.maximum(
                jnp.where(near2, lanes_max(tile), LOW),
                jnp.where(near2_partner, lanes_max(other), LOW))
            top = jnp.max(tile, axis=0, keepdims=True)
            best[0:1, :] = jnp.maximum(best[0:1, :], jnp.where(near2, top, LOW))
            top = jnp.max(other, axis=0, keepdims=True)
            best[1:2, :] = jnp.maximum(best[1:2, :], jnp.where(near2_partner, top, LOW))

    @pl.when(has_earlier)
    def _():
        ret_out[...] = jnp.max(row_two[...].T, axis=0, keepdims=True)
        part_out[...] = best[1:2, :]
        small(0, ret_out, ret_in, me - 2).start()
        small(1, part_out, part_in, partner).start()

    @pl.when(has_earlier3)
    def _():
        top = jnp.max(row_three[...].T, axis=0, keepdims=True)
        ret3_out[...] = jnp.where(near3, top, LOW)
        small(2, ret3_out, ret3_in, me - 3).start()

    @pl.when(has_earlier)
    def _():
        small(1, part_out, part_in, partner).wait()
        best[0:1, :] = jnp.maximum(best[0:1, :], part_in[...])

    @pl.when(has_later3)
    def _():
        small(2, ret3_out, ret3_in, me + 3).wait_recv()
        best[0:1, :] = jnp.maximum(best[0:1, :], ret3_in[...])

    @pl.when(has_later)
    def _():
        small(0, ret_out, ret_in, me + 2).wait_recv()
        best[0:1, :] = jnp.maximum(best[0:1, :], ret_in[...])

    out_ref[...] = best[0:1, :]

    @pl.loop(0, PIECES)
    def _(q):
        @pl.when(has_later3)
        def _():
            to_three(q).wait_send()

        @pl.when(sends_direct)
        def _():
            to_two(q).wait_send()

        @pl.when(relays)
        def _():
            onward(q).wait_send()

    @pl.when(has_earlier)
    def _():
        small(0, ret_out, ret_in, me - 2).wait_send()

    @pl.when(has_earlier3)
    def _():
        small(2, ret3_out, ret3_in, me - 3).wait_send()


def shards(sizes, embeddings, cluster_blocks):
    block, width = embeddings.shape
    line = pltpu.VMEM((1, block), jnp.float32)
    wide = pltpu.VMEM((block, width), jnp.bfloat16)
    flags = pltpu.SemaphoreType.DMA((PIECES,))
    lone = pltpu.SemaphoreType.DMA
    out = pl.pallas_call(
        functools.partial(nearest_kernel, sizes),
        out_shape=pltpu.VMEM((1, block), jnp.float32),
        in_specs=[pl.BlockSpec(memory_space=pl.ANY)] * 2,
        out_specs=pl.BlockSpec(memory_space=pltpu.VMEM),
        scratch_shapes=[
            wide, pltpu.VMEM((2, block, width), jnp.bfloat16), wide, wide,
            pltpu.VMEM((block, 128), jnp.float32), pltpu.VMEM((block, 128), jnp.float32),
            pltpu.VMEM((8, block), jnp.float32),
            line, line, line, line, line, line,
            lone, lone, lone, flags, flags, flags, flags,
            pltpu.SemaphoreType.DMA((3,)), pltpu.SemaphoreType.DMA((3,)),
            pltpu.SMEM(cluster_blocks.shape, jnp.int32), lone,
        ],
        compiler_params=pltpu.CompilerParams(collective_id=0, has_side_effects=True),
        name="nearest",
    )(cluster_blocks, embeddings)
    return out.reshape(-1)


def solution(mesh):
    sizes = (mesh.shape["rows"], mesh.shape["bal"])
    return jax.shard_map(
        functools.partial(shards, sizes), mesh=mesh,
        in_specs=(P(("rows", "bal"), None), P()), out_specs=P(("rows", "bal")), check_vma=False)
```

```python
import functools

import jax
import jax.numpy as jnp
from jax import lax
from jax.experimental import pallas as pl
from jax.experimental.pallas import tpu as pltpu
from jax.sharding import PartitionSpec as P

EPSILON = 1e-06
LOW = -2.0
MESH_ID = pl.DeviceIdType.MESH
PIECES = 8


def nearest_kernel(sizes, counts_hbm, x_ref, out_ref, raw, pair, two_back, three_back,
                   row_two, row_three, best, part_out, ret_out, ret3_out, part_in, ret_in, ret3_in,
                   load_sem, pair_send, pair_recv, two_send, two_recv, three_send, three_recv,
                   small_send, small_recv, counts_ref, counts_sem):
    n_rows, n_bal = sizes
    total = n_rows * n_bal
    block, width = x_ref.shape
    piece = block // PIECES
    me = lax.axis_index("rows") * n_bal + lax.axis_index("bal")
    odd = lax.rem(me, 2)
    quarter = lax.rem(me, 4)
    partner = me + 1 - 2 * odd
    is_even = odd == 0
    is_odd = odd == 1

    has_later = me + 2 < total
    has_earlier = me >= 2
    has_later3 = is_odd & (me + 3 < total)
    has_earlier3 = is_even & (me >= 3)
    sends_direct = has_later & ((quarter != 3) | (me + 3 >= total))
    relays = has_earlier3 & (quarter == 2)
    relayed_to = has_earlier & (quarter == 1) & (me + 1 < total)

    def coords(index):
        return (index // n_bal, lax.rem(index, n_bal))

    barrier = pltpu.get_barrier_semaphore()
    greeted = jnp.int32(0)
    for there, index in (
        (me >= 0, partner),
        (has_later, me + 2),
        (has_earlier, me - 2),
        (has_later3, me + 3),
        (has_earlier3, me - 3),
        (relays, me - 1),
        (relayed_to, me + 1),
    ):
        @pl.when(there)
        def _():
            pl.semaphore_signal(barrier, inc=1, device_id=coords(index), device_id_type=MESH_ID)
        greeted = greeted + there.astype(jnp.int32)

    def load(q):
        rows = pl.ds(pl.multiple_of(q * piece, piece), piece)
        return pltpu.make_async_copy(x_ref.at[rows], raw.at[rows], load_sem.at[q])

    @pl.loop(0, PIECES)
    def _(q):
        load(q).start()

    counts_load = pltpu.make_async_copy(counts_hbm, counts_ref, counts_sem)
    counts_load.start()


    @pl.loop(0, PIECES)
    def _(q):
        rows = pl.ds(pl.multiple_of(q * piece, piece), piece)
        load(q).wait()
        values = raw[rows, :].astype(jnp.float32)
        scale = lax.rsqrt(jnp.sum(values * values, axis=1, keepdims=True) + EPSILON)
        pair[0, rows, :] = (values * scale).astype(jnp.bfloat16)

    pl.semaphore_wait(barrier, greeted)

    def rows_of(q):
        return pl.ds(pl.multiple_of(q * piece, piece), piece)

    def to_two(q):
        return pltpu.make_async_remote_copy(
            src_ref=pair.at[0, rows_of(q)], dst_ref=two_back.at[rows_of(q)],
            send_sem=two_send.at[q], recv_sem=two_recv.at[q],
            device_id=coords(me + 2), device_id_type=MESH_ID)

    def to_three(q):
        return pltpu.make_async_remote_copy(
            src_ref=pair.at[0, rows_of(q)], dst_ref=three_back.at[rows_of(q)],
            send_sem=three_send.at[q], recv_sem=three_recv.at[q],
            device_id=coords(me + 3), device_id_type=MESH_ID)

    def onward(q):
        return pltpu.make_async_remote_copy(
            src_ref=three_back.at[rows_of(q)], dst_ref=two_back.at[rows_of(q)],
            send_sem=three_send.at[q], recv_sem=two_recv.at[q],
            device_id=coords(me - 1), device_id_type=MESH_ID)

    def to_partner():
        return pltpu.make_async_remote_copy(
            src_ref=pair.at[0], dst_ref=pair.at[1],
            send_sem=pair_send, recv_sem=pair_recv,
            device_id=coords(partner), device_id_type=MESH_ID)

    def small(slot, src, dst, index):
        return pltpu.make_async_remote_copy(
            src_ref=src, dst_ref=dst, send_sem=small_send.at[slot], recv_sem=small_recv.at[slot],
            device_id=coords(index), device_id_type=MESH_ID)

    to_partner().start()

    @pl.loop(0, PIECES)
    def _(q):
        @pl.when(has_later3)
        def _():
            to_three(q).start()

        @pl.when(sends_direct)
        def _():
            to_two(q).start()

    counts_load.wait()

    def count(i, carry):
        end, crossings = carry
        end = end + counts_ref[i]
        found = []
        for (lower, upper), old in zip(spans, crossings):
            found.append(old + ((end > lower) & (end <= upper)).astype(jnp.int32))
        return end, tuple(found)

    spans = ((me - 3, me), (me - 2, me), (me - 1, me), (me, me + 1), (me - 2, partner))
    zero = jnp.int32(0)
    _, crossings = lax.fori_loop(0, counts_ref.shape[0], count, (zero, (zero,) * len(spans)))
    near3 = crossings[0] == 0
    near2 = crossings[1] == 0
    near_partner = jnp.where(is_odd, crossings[2], crossings[3]) == 0
    near2_partner = crossings[4] == 0

    def products(left, right):
        return lax.dot_general(left, right, (((1,), (1,)), ((), ())),
                               preferred_element_type=jnp.float32)

    step = 128
    best[...] = jnp.full(best.shape, LOW, jnp.float32)

    @pl.loop(0, block // step)
    def _(s):
        rows = pl.ds(pl.multiple_of(s * step, step), step)
        own = products(pair[0, rows, :], pair[0])
        across = lax.broadcasted_iota(jnp.int32, own.shape, 1)
        down = lax.broadcasted_iota(jnp.int32, own.shape, 0) + s * step
        own = jnp.where(across == down, LOW, own)
        best[0:1, :] = jnp.maximum(best[0:1, :], jnp.max(own, axis=0, keepdims=True))

    to_partner().wait()

    @pl.loop(0, block // step)
    def _(s):
        rows = pl.ds(pl.multiple_of(s * step, step), step)
        other = products(pair[1, rows, :], pair[0])
        top = jnp.max(other, axis=0, keepdims=True)
        best[0:1, :] = jnp.maximum(best[0:1, :], jnp.where(near_partner, top, LOW))

    def lanes_max(tile):
        highest = tile[:, :128]
        for start in range(128, tile.shape[1], 128):
            highest = jnp.maximum(highest, tile[:, start:start + 128])
        return highest

    @pl.loop(0, PIECES)
    def _(q):
        rows = rows_of(q)

        @pl.when(has_earlier3)
        def _():
            to_three(q).wait_recv()

            @pl.when(relays)
            def _():
                onward(q).start()

            tile = products(three_back[rows, :], pair[0])
            row_three[rows, :] = lanes_max(tile)
            top = jnp.max(tile, axis=0, keepdims=True)
            best[0:1, :] = jnp.maximum(best[0:1, :], jnp.where(near3, top, LOW))

        @pl.when(has_earlier)
        def _():
            to_two(q).wait_recv()
            tile = products(two_back[rows, :], pair[0])
            other = products(two_back[rows, :], pair[1])
            row_two[rows, :] = jnp.maximum(
                jnp.where(near2, lanes_max(tile), LOW),
                jnp.where(near2_partner, lanes_max(other), LOW))
            top = jnp.max(tile, axis=0, keepdims=True)
            best[0:1, :] = jnp.maximum(best[0:1, :], jnp.where(near2, top, LOW))
            top = jnp.max(other, axis=0, keepdims=True)
            best[1:2, :] = jnp.maximum(best[1:2, :], jnp.where(near2_partner, top, LOW))

    @pl.when(has_earlier)
    def _():
        ret_out[...] = jnp.max(row_two[...].T, axis=0, keepdims=True)
        part_out[...] = best[1:2, :]
        small(0, ret_out, ret_in, me - 2).start()
        small(1, part_out, part_in, partner).start()

    @pl.when(has_earlier3)
    def _():
        top = jnp.max(row_three[...].T, axis=0, keepdims=True)
        ret3_out[...] = jnp.where(near3, top, LOW)
        small(2, ret3_out, ret3_in, me - 3).start()

    @pl.when(has_earlier)
    def _():
        small(1, part_out, part_in, partner).wait()
        best[0:1, :] = jnp.maximum(best[0:1, :], part_in[...])

    @pl.when(has_later3)
    def _():
        small(2, ret3_out, ret3_in, me + 3).wait_recv()
        best[0:1, :] = jnp.maximum(best[0:1, :], ret3_in[...])

    @pl.when(has_later)
    def _():
        small(0, ret_out, ret_in, me + 2).wait_recv()
        best[0:1, :] = jnp.maximum(best[0:1, :], ret_in[...])

    out_ref[...] = best[0:1, :]

    @pl.loop(0, PIECES)
    def _(q):
        @pl.when(has_later3)
        def _():
            to_three(q).wait_send()

        @pl.when(sends_direct)
        def _():
            to_two(q).wait_send()

        @pl.when(relays)
        def _():
            onward(q).wait_send()

    @pl.when(has_earlier)
    def _():
        small(0, ret_out, ret_in, me - 2).wait_send()

    @pl.when(has_earlier3)
    def _():
        small(2, ret3_out, ret3_in, me - 3).wait_send()


def shards(sizes, embeddings, cluster_blocks):
    block, width = embeddings.shape
    line = pltpu.VMEM((1, block), jnp.float32)
    wide = pltpu.VMEM((block, width), jnp.bfloat16)
    flags = pltpu.SemaphoreType.DMA((PIECES,))
    lone = pltpu.SemaphoreType.DMA
    out = pl.pallas_call(
        functools.partial(nearest_kernel, sizes),
        out_shape=pltpu.VMEM((1, block), jnp.float32),
        in_specs=[pl.BlockSpec(memory_space=pl.ANY)] * 2,
        out_specs=pl.BlockSpec(memory_space=pltpu.VMEM),
        scratch_shapes=[
            wide, pltpu.VMEM((2, block, width), jnp.bfloat16), wide, wide,
            pltpu.VMEM((block, 128), jnp.float32), pltpu.VMEM((block, 128), jnp.float32),
            pltpu.VMEM((8, block), jnp.float32),
            line, line, line, line, line, line,
            flags, lone, lone, flags, flags, flags, flags,
            pltpu.SemaphoreType.DMA((3,)), pltpu.SemaphoreType.DMA((3,)),
            pltpu.SMEM(cluster_blocks.shape, jnp.int32), lone,
        ],
        compiler_params=pltpu.CompilerParams(collective_id=0, has_side_effects=True),
        name="nearest",
    )(cluster_blocks, embeddings)
    return out.reshape(-1)


def solution(mesh):
    sizes = (mesh.shape["rows"], mesh.shape["bal"])
    return jax.shard_map(
        functools.partial(shards, sizes), mesh=mesh,
        in_specs=(P(("rows", "bal"), None), P()), out_specs=P(("rows", "bal")), check_vma=False)
```
